32 devices in a mesh: row: 8 (over y, x, core), col: 4 (over z).
Axes of the slice: x: 2, y: 2, z: 4, core: 2. Of those that a mesh axis runs over, the one named last changes fastest.
Arguments:
- queries: bfloat16 [8, 128, 4096], P(None, 'row', 'col'), may hold values from -13 to 13, as said below
- key_cache: bfloat16 [8, 16384, 1024], P(None, ('row', 'col')), may hold values from -13 to 13
- value_cache: bfloat16 [8, 16384, 1024], P(None, ('row', 'col')), may hold values from -6 to 6
- key_table: bfloat16 [1024, 1024], replicated, may hold values from -24 to 24
- value_table: bfloat16 [1024, 1024], replicated, may hold values from -6 to 6
- lengths: int32 [8], replicated, may hold values from 2048 to 16384
- token_ids: int32 [8, 128], P(None, 'row'), may hold values from 0 to 1023
Outputs:
- attended: bfloat16 [8, 128, 4096], P(None, 'row', 'col')
The draws below stay inside these ranges and needn't reach their ends.
Inputs may be any that keep to these rules, and one draw needn't show every extreme that they name: `queries`: entries of the query array lie in the stated range.
All inputs are finite; a program needn't handle non-finite values.
Results may differ from the reference program's by a relative error of at most 0.006.
Values may be sent and summed in bfloat16 or wider, within the bound.
A program may use at most 192 MiB of HBM per device.

```python
import jax
import jax.numpy as jnp
from jax import lax

USERS = 8
BEAMS = 128
L_DEV = 512
HQ = 32
KH = 8
HD = 128
VOCAB = 1024
CONTEXT = 16384


def anchor_parts(key):
    signs = jnp.where(jax.random.bernoulli(jax.random.fold_in(key, 4242), 0.5, (USERS, KH, HD)), 1.7, -1.7)
    places = jax.random.randint(jax.random.fold_in(key, 4243), (USERS,), 0, CONTEXT // 8 - 1)
    strength = jax.random.uniform(jax.random.fold_in(key, 4244), (USERS,), jnp.float32, 1.5, 4.0)
    return (signs.astype(jnp.float32), places, strength)


def draw_key_cache(key, part):
    base = jnp.clip(jax.random.normal(jax.random.fold_in(key, 11), (USERS, CONTEXT, KH * HD), jnp.float32), -6.0, 6.0)
    anchors, places, strength = anchor_parts(key)
    flat = anchors.reshape(USERS, 1, KH * HD)
    spots = jnp.arange(CONTEXT, dtype=jnp.int32)[None, :, None]
    base = jnp.where(spots == places[:, None, None], 4.0 * flat, base)
    base = jnp.where(spots == places[:, None, None] + 1, 3.96 * flat, base)
    return jnp.clip(base, -13.0, 13.0).astype(jnp.bfloat16)


def draw_queries(key, part):
    base = jnp.clip(jax.random.normal(jax.random.fold_in(key, 21), (USERS, BEAMS, HQ * HD), jnp.float32), -6.0, 6.0)
    anchors, places, strength = anchor_parts(key)
    factor = strength * (81.0 / (11.56 * HD ** 0.5))
    spread = jnp.repeat(anchors, HQ // KH, axis=1).reshape(USERS, 1, HQ * HD) * factor[:, None, None]
    beam_at = jnp.arange(BEAMS, dtype=jnp.int32)[None, :, None]
    base = jnp.where(beam_at == 0, spread, base)
    return jnp.clip(base, -13.0, 13.0).astype(jnp.bfloat16)


def set_ends(entries, rng, least, high):
    extent = entries.shape
    index_at = [jax.random.randint(jax.random.fold_in(rng, axis), (), 0, extent[axis]) for axis in range(len(extent))]
    entries = entries.at[tuple(index_at)].set(least)
    longest = extent.index(max(extent))
    index_at[longest] = (index_at[longest] + 1) % extent[longest]
    return entries.at[tuple(index_at)].set(high)


def levels(key, shape, pieces, least, top_value):
    def one(dim, parts):
        draws = jax.random.uniform(jax.random.fold_in(jax.random.fold_in(key, 6), dim), (parts,), jnp.float32, least / len(pieces), top_value / len(pieces))
        return jnp.repeat(jnp.exp(draws), shape[dim] // parts).reshape((-1,) + (1,) * (len(shape) - dim - 1))

    level = one(*pieces[0])
    for cut in pieces[1:]:
        level = level * one(*cut)
    return level


def noise(own_key, dims, width, reach, shards=(), held_as=jnp.bfloat16):
    level = levels(own_key, dims, shards, -0.22, 0.18) if shards else 1.0
    array = jax.random.normal(own_key, dims, jnp.float32) * width * level
    return jnp.minimum(jnp.maximum(array, -reach), reach).astype(held_as)


def setup_inputs(seed: int = 0) -> dict:
    streams_of = jax.random.split(jax.random.key(seed), 8)
    queries = draw_queries(jax.random.fold_in(streams_of[7], 71), 0)
    key_cache = draw_key_cache(jax.random.fold_in(streams_of[7], 71), 0)
    value_cache = noise(streams_of[2], (USERS, CONTEXT, KH * HD), 1.0, 6.0, ((1, 32),))
    key_table = noise(streams_of[3], (VOCAB, KH * HD), 4.0, 24.0)
    value_table = noise(streams_of[4], (VOCAB, KH * HD), 1.0, 6.0)
    lengths = set_ends(jax.random.randint(streams_of[5], (USERS,), CONTEXT // 8, CONTEXT + 1), jax.random.fold_in(streams_of[5], 1), CONTEXT // 8, CONTEXT).astype(jnp.int32)
    token_ids = set_ends(jax.random.randint(streams_of[6], (USERS, BEAMS), 0, VOCAB), jax.random.fold_in(streams_of[6], 1), 0, VOCAB - 1).astype(jnp.int32)
    return dict(queries=queries, key_cache=key_cache, value_cache=value_cache, key_table=key_table, value_table=value_table, lengths=lengths, token_ids=token_ids)


def reference(queries, key_cache, value_cache, key_table, value_table, lengths, token_ids):
    group = HQ // KH
    scale = HD ** -0.5
    blocks = CONTEXT // L_DEV
    q_all = queries.astype(jnp.float32).reshape(USERS, BEAMS, KH, group, HD)
    own_keys = key_table[token_ids].astype(jnp.float32).reshape(USERS, BEAMS, KH, 1, HD)
    own_values = value_table[token_ids].astype(jnp.float32).reshape(USERS, BEAMS, KH, 1, HD)
    own_scores = jnp.sum(q_all * own_keys, axis=-1) * scale
    starts = jnp.arange(blocks, dtype=jnp.int32) * L_DEV

    def per_user(items):
        q_user, k_user, v_user, limit, self_score, self_value = items
        k_blocks = k_user.reshape(blocks, L_DEV, KH, HD)
        v_blocks = v_user.reshape(blocks, L_DEV, KH, HD)

        def scores(k_blk, start):
            s = jnp.einsum('wkgd,lkd->wkgl', q_user, k_blk.astype(jnp.float32)) * scale
            live = (start + jnp.arange(L_DEV, dtype=jnp.int32)) < limit
            return jnp.where(live, s, -1e30), live

        def pass_max(peak, items):
            k_blk, start = items
            s, live = scores(k_blk, start)
            return jnp.maximum(peak, jnp.max(s, axis=-1)), None

        peak, _ = lax.scan(pass_max, self_score, (k_blocks, starts))
        first = jnp.exp(self_score - peak)

        def pass_sum(carry, items):
            total, numer = carry
            k_blk, v_blk, start = items
            s, live = scores(k_blk, start)
            weight = jnp.where(live, jnp.exp(s - peak[..., None]), 0.0)
            total = total + jnp.sum(weight, axis=-1)
            rounded = weight.astype(jnp.bfloat16).astype(jnp.float32)
            numer = numer + jnp.einsum('wkgl,lkd->wkgd', rounded, v_blk.astype(jnp.float32))
            return (total, numer), None

        init = (first, first[..., None] * self_value)
        (total, numer), _ = lax.scan(pass_sum, init, (k_blocks, v_blocks, starts))
        return (numer / total[..., None]).reshape(BEAMS, HQ * HD).astype(jnp.bfloat16)

    return lax.map(per_user, (q_all, key_cache, value_cache, lengths, own_scores, own_values))
```

```python
import functools
import math

import jax
import jax.numpy as jnp
from jax import lax
from jax.experimental import pallas as pl
from jax.experimental.pallas import tpu as pltpu
from jax.sharding import PartitionSpec as P

HQ = 32
KH = 8
HD = 128
GROUP = HQ // KH
CHUNKS = 2
LOG2E = math.log2(math.e)
MESH = pl.DeviceIdType.MESH


def attend_kernel(live_ref, q_ref, k_ref, v_ref, o_ref, m_ref, l_ref):
    rows, cols, _, piece, _ = q_ref.shape
    positions = k_ref.shape[1]
    kv_part = KH // cols
    part = piece // kv_part
    factor = HD ** (-0.5) * LOG2E
    live = live_ref[pl.program_id(0)]

    def run(masked):
        if masked:
            keep = lax.broadcasted_iota(jnp.int32, (positions, rows * part), 0) < live
        for j in range(KH):
            c, at = divmod(j, kv_part)
            span = slice(at * part, (at + 1) * part)
            q = q_ref[:, c, 0, span, :].reshape(rows * part, HD)
            k = k_ref[0, :, j * HD : (j + 1) * HD]
            s = lax.dot_general(k, q, (((1,), (1,)), ((), ())), preferred_element_type=jnp.float32)
            if masked:
                s = jnp.where(keep, s, -1e30)
            m = jnp.max(s, axis=0, keepdims=True)
            p = jnp.exp2((s - m) * factor)
            l_ref[0, j : j + 1, :] = jnp.sum(p, axis=0, keepdims=True)
            m_ref[0, j : j + 1, :] = m * factor
            v = v_ref[0, :, j * HD : (j + 1) * HD]
            o = lax.dot_general(
                v, p.astype(jnp.bfloat16), (((0,), (0,)), ((), ())), preferred_element_type=jnp.float32
            )
            o_ref[:, c, 0, span, :] = o.T.astype(jnp.bfloat16).reshape(rows, part, HD)

    @pl.when(live >= positions)
    def _():
        run(False)

    @pl.when((live > 0) & (live < positions))
    def _():
        run(True)

    @pl.when(live <= 0)
    def _():
        o_ref[...] = jnp.zeros_like(o_ref)
        m_ref[...] = jnp.full_like(m_ref, -1e30)
        l_ref[...] = jnp.zeros_like(l_ref)


def attend(live, gathered, keys, values, first):
    rows, cols, users, piece, _ = gathered.shape
    _, positions, width = keys.shape
    stat = rows * piece * cols // KH
    q_spec = pl.BlockSpec((rows, cols, 1, piece, HD), lambda u, live: (0, 0, u, 0, 0))
    c_spec = pl.BlockSpec((1, positions, width), lambda u, live: (u + first, 0, 0))
    s_spec = pl.BlockSpec((1, KH, stat), lambda u, live: (u, 0, 0))
    scores = users * KH * stat * positions
    return pl.pallas_call(
        attend_kernel,
        grid_spec=pltpu.PrefetchScalarGridSpec(
            num_scalar_prefetch=1,
            grid=(users,),
            in_specs=[q_spec, c_spec, c_spec],
            out_specs=[q_spec, s_spec, s_spec],
        ),
        out_shape=[
            jax.ShapeDtypeStruct(gathered.shape, jnp.bfloat16),
            jax.ShapeDtypeStruct((users, KH, stat), jnp.float32),
            jax.ShapeDtypeStruct((users, KH, stat), jnp.float32),
        ],
        compiler_params=pltpu.CompilerParams(
            dimension_semantics=("arbitrary",), vmem_limit_bytes=40 * 1024 * 1024
        ),
        cost_estimate=pl.CostEstimate(
            flops=4 * scores * HD * 2,
            bytes_accessed=4 * gathered.size + 4 * users * positions * width,
            transcendentals=scores,
        ),
        name="attend",
    )(live, gathered, keys, values)


def merge(pieces, n):
    peak = functools.reduce(jnp.maximum, [x[:n] for x in pieces])
    total = sum(x[n:] * jnp.exp2(x[:n] - peak) for x in pieces)
    return peak, total


def peaks_kernel(
    st_ref, all_ref, own_ref, row_in, col_out, col_in, row_all, send_sem, recv_sem
):
    rows, cols, two, _ = st_ref.shape
    n = two // 2
    me = {"row": lax.axis_index("row"), "col": lax.axis_index("col")}
    size = {"row": rows, "col": cols}

    def peer(axis, step):
        return {axis: lax.rem(me[axis] + step, size[axis])}

    others = [(axis, step) for axis in ("row", "col") for step in range(1, size[axis])]
    barrier = pltpu.get_barrier_semaphore()
    for axis, step in others:
        pl.semaphore_signal(barrier, inc=1, device_id=peer(axis, step), device_id_type=MESH)
    pl.semaphore_wait(barrier, len(others))

    taken = [0]

    def exchange(axis, source, target):
        copies = []
        for step in range(1, size[axis]):
            to = peer(axis, step)
            copy = pltpu.make_async_remote_copy(
                src_ref=source(to[axis]),
                dst_ref=target(step),
                send_sem=send_sem.at[taken[0]],
                recv_sem=recv_sem.at[taken[0]],
                device_id=to,
                device_id_type=MESH,
            )
            taken[0] += 1
            copy.start()
            copies.append(copy)
        for copy in copies:
            copy.wait()

    exchange("row", lambda to: st_ref.at[to], lambda step: row_in.at[step - 1])
    mine = st_ref[me["row"]]
    for c in range(cols):
        peak, total = merge([mine[c]] + [row_in[step, c] for step in range(rows - 1)], n)
        col_out[c, :n] = peak
        col_out[c, n:] = total
    exchange("col", lambda to: col_out.at[to], lambda step: col_in.at[step - 1])
    peak, total = merge([col_out[me["col"]]] + [col_in[step] for step in range(cols - 1)], n)
    own_ref[:n] = peak
    own_ref[n:] = total
    here = row_all.at[me["row"]]
    here[me["col"]] = peak
    spot = here.at[me["col"]]
    exchange("col", lambda to: spot, lambda step: spot)
    exchange("row", lambda to: here, lambda step: here)
    all_ref[...] = row_all[...]


def peaks(stats):
    rows, cols, two, lanes = stats.shape
    n = two // 2
    sends = 2 * (rows - 1) + 2 * (cols - 1)
    vmem = pl.BlockSpec(memory_space=pltpu.VMEM)
    return pl.pallas_call(
        peaks_kernel,
        out_shape=[
            jax.ShapeDtypeStruct((rows, cols, n, lanes), jnp.float32),
            jax.ShapeDtypeStruct((two, lanes), jnp.float32),
        ],
        in_specs=[vmem],
        out_specs=[vmem, vmem],
        scratch_shapes=[
            pltpu.VMEM((rows - 1, cols, two, lanes), jnp.float32),
            pltpu.VMEM((cols, two, lanes), jnp.float32),
            pltpu.VMEM((cols - 1, two, lanes), jnp.float32),
            pltpu.VMEM((rows, cols, n, lanes), jnp.float32),
            pltpu.SemaphoreType.DMA((sends,)),
            pltpu.SemaphoreType.DMA((sends,)),
        ],
        compiler_params=pltpu.CompilerParams(collective_id=0, has_side_effects=True),
        name="peaks",
    )(stats)


def body(queries, key_cache, value_cache, key_table, value_table, lengths, token_ids):
    users, beam_part, width_part = queries.shape
    heads_part = width_part // HD
    kv_part = heads_part // GROUP
    rows, cols = lax.axis_size("row"), lax.axis_size("col")
    row_at, col_at = lax.axis_index("row"), lax.axis_index("col")
    positions = key_cache.shape[1]
    offset = (row_at * cols + col_at) * positions
    live = jnp.clip(lengths - offset, 0, positions)
    piece = heads_part * beam_part
    q_local = queries.reshape(users, beam_part, heads_part, HD).transpose(0, 2, 1, 3)
    q_local = q_local.reshape(users, piece, HD)
    some = users // CHUNKS

    gathered = [
        lax.all_gather(q_local[i * some : (i + 1) * some], ("row", "col"), axis=0)
        for i in range(CHUNKS)
    ]

    own_keys, own_values = (
        jnp.einsum(
            "uwv,vc->uwc",
            (token_ids[..., None] == jnp.arange(table.shape[0], dtype=jnp.int32)).astype(jnp.bfloat16),
            lax.dynamic_slice_in_dim(table, col_at * kv_part * HD, kv_part * HD, 1),
            preferred_element_type=jnp.float32,
        )
        .reshape(users, beam_part, kv_part, HD)
        .transpose(0, 2, 1, 3)[:, :, None]
        for table in (key_table, value_table)
    )
    q_heads = q_local.astype(jnp.float32).reshape(users, kv_part, GROUP, beam_part, HD)
    own_score = jnp.sum(q_heads * own_keys, axis=-1) * (HD ** (-0.5) * LOG2E)

    outs = []
    for i in range(CHUNKS):
        span = slice(i * some, (i + 1) * some)
        numer, m, l = attend(
            live[span],
            gathered[i].reshape(rows, cols, some, piece, HD),
            key_cache,
            value_cache,
            i * some,
        )

        def by_device(x):
            x = x.reshape(some, cols, kv_part, rows, piece // kv_part)
            return x.transpose(3, 1, 0, 2, 4).reshape(rows, cols, some * piece // HD, HD)

        m = by_device(m)
        peak_all, own = peaks(jnp.concatenate([m, by_device(l)], axis=2))
        factor = jnp.exp2(m - peak_all).reshape(rows * cols, some, piece)
        weighted = numer.reshape(rows * cols, some, piece, HD).astype(jnp.float32) * factor[..., None]
        numer = lax.psum_scatter(
            weighted.astype(jnp.bfloat16), ("row", "col"), scatter_dimension=0, tiled=False
        )
        numer = numer.astype(jnp.float32).reshape(some, kv_part, GROUP, beam_part, HD)
        peak, total = own.reshape(2, some, kv_part, GROUP, beam_part)
        e = own_score[span]
        top = jnp.maximum(peak, e)
        carried = jnp.exp2(peak - top)
        fresh = jnp.exp2(e - top)
        numer = numer * carried[..., None] + fresh[..., None] * own_values[span]
        outs.append(numer / (total * carried + fresh)[..., None])
    result = jnp.concatenate(outs).reshape(users, heads_part, beam_part, HD)
    return result.transpose(0, 2, 1, 3).reshape(users, beam_part, width_part).astype(jnp.bfloat16)


def solution(mesh):
    return jax.shard_map(
        body,
        mesh=mesh,
        in_specs=(
            P(None, "row", "col"),
            P(None, ("row", "col"), None),
            P(None, ("row", "col"), None),
            P(),
            P(),
            P(),
            P(None, "row"),
        ),
        out_specs=P(None, "row", "col"),
        check_vma=False,
    )
```

```python
import functools
import math

import jax
import jax.numpy as jnp
from jax import lax
from jax.experimental import pallas as pl
from jax.experimental.pallas import tpu as pltpu
from jax.sharding import PartitionSpec as P

HQ = 32
KH = 8
HD = 128
GROUP = HQ // KH
CHUNKS = 2
LOG2E = math.log2(math.e)
MESH = pl.DeviceIdType.MESH


def attend_kernel(live_ref, q_ref, k_ref, v_ref, o_ref, m_ref, l_ref):
    rows, cols, _, piece, _ = q_ref.shape
    positions = k_ref.shape[1]
    kv_part = KH // cols
    part = piece // kv_part
    factor = HD ** (-0.5) * LOG2E
    live = live_ref[pl.program_id(0)]

    def run(masked):
        if masked:
            keep = lax.broadcasted_iota(jnp.int32, (positions, rows * part), 0) < live
        for j in range(KH):
            c, at = divmod(j, kv_part)
            span = slice(at * part, (at + 1) * part)
            q = q_ref[:, c, 0, span, :].reshape(rows * part, HD)
            k = k_ref[0, :, j * HD : (j + 1) * HD]
            s = lax.dot_general(k, q, (((1,), (1,)), ((), ())), preferred_element_type=jnp.float32)
            if masked:
                s = jnp.where(keep, s, -1e30)
            m = jnp.max(s, axis=0, keepdims=True)
            p = jnp.exp2((s - m) * factor)
            l_ref[0, j : j + 1, :] = jnp.sum(p, axis=0, keepdims=True)
            m_ref[0, j : j + 1, :] = m * factor
            v = v_ref[0, :, j * HD : (j + 1) * HD]
            o = lax.dot_general(
                v, p.astype(jnp.bfloat16), (((0,), (0,)), ((), ())), preferred_element_type=jnp.float32
            )
            o_ref[:, c, 0, span, :] = o.T.astype(jnp.bfloat16).reshape(rows, part, HD)

    @pl.when(live >= positions)
    def _():
        run(False)

    @pl.when((live > 0) & (live < positions))
    def _():
        run(True)

    @pl.when(live <= 0)
    def _():
        o_ref[...] = jnp.zeros_like(o_ref)
        m_ref[...] = jnp.full_like(m_ref, -1e30)
        l_ref[...] = jnp.zeros_like(l_ref)


def attend(live, gathered, keys, values, first):
    rows, cols, users, piece, _ = gathered.shape
    _, positions, width = keys.shape
    stat = rows * piece * cols // KH
    q_spec = pl.BlockSpec((rows, cols, 1, piece, HD), lambda u, live: (0, 0, u, 0, 0))
    c_spec = pl.BlockSpec((1, positions, width), lambda u, live: (u + first, 0, 0))
    s_spec = pl.BlockSpec((1, KH, stat), lambda u, live: (u, 0, 0))
    scores = users * KH * stat * positions
    return pl.pallas_call(
        attend_kernel,
        grid_spec=pltpu.PrefetchScalarGridSpec(
            num_scalar_prefetch=1,
            grid=(users,),
            in_specs=[q_spec, c_spec, c_spec],
            out_specs=[q_spec, s_spec, s_spec],
        ),
        out_shape=[
            jax.ShapeDtypeStruct(gathered.shape, jnp.bfloat16),
            jax.ShapeDtypeStruct((users, KH, stat), jnp.float32),
            jax.ShapeDtypeStruct((users, KH, stat), jnp.float32),
        ],
        compiler_params=pltpu.CompilerParams(
            dimension_semantics=("arbitrary",), vmem_limit_bytes=40 * 1024 * 1024
        ),
        cost_estimate=pl.CostEstimate(
            flops=4 * scores * HD * 2,
            bytes_accessed=4 * gathered.size + 4 * users * positions * width,
            transcendentals=scores,
        ),
        name="attend",
    )(live, gathered, keys, values)


def merge(pieces, n):
    peak = functools.reduce(jnp.maximum, [x[:n] for x in pieces])
    total = sum(x[n:] * jnp.exp2(x[:n] - peak) for x in pieces)
    return peak, total


def peaks_kernel(
    st_ref, all_ref, own_ref, row_in, col_out, col_in, row_all, send_sem, recv_sem
):
    rows, cols, two, _ = st_ref.shape
    n = two // 2
    me = {"row": lax.axis_index("row"), "col": lax.axis_index("col")}
    size = {"row": rows, "col": cols}

    def peer(axis, step):
        return {axis: lax.rem(me[axis] + step, size[axis])}

    others = [(axis, step) for axis in ("row", "col") for step in range(1, size[axis])]
    barrier = pltpu.get_barrier_semaphore()
    for axis, step in others:
        pl.semaphore_signal(barrier, inc=1, device_id=peer(axis, step), device_id_type=MESH)
    pl.semaphore_wait(barrier, len(others))

    taken = [0]

    def exchange(axis, source, target):
        copies = []
        for step in range(1, size[axis]):
            to = peer(axis, step)
            copy = pltpu.make_async_remote_copy(
                src_ref=source(to[axis]),
                dst_ref=target(step),
                send_sem=send_sem.at[taken[0]],
                recv_sem=recv_sem.at[taken[0]],
                device_id=to,
                device_id_type=MESH,
            )
            taken[0] += 1
            copy.start()
            copies.append(copy)
        for copy in copies:
            copy.wait()

    exchange("row", lambda to: st_ref.at[to], lambda step: row_in.at[step - 1])
    mine = st_ref[me["row"]]
    for c in range(cols):
        peak, total = merge([mine[c]] + [row_in[step, c] for step in range(rows - 1)], n)
        col_out[c, :n] = peak
        col_out[c, n:] = total
    exchange("col", lambda to: col_out.at[to], lambda step: col_in.at[step - 1])
    peak, total = merge([col_out[me["col"]]] + [col_in[step] for step in range(cols - 1)], n)
    own_ref[:n] = peak
    own_ref[n:] = total
    here = row_all.at[me["row"]]
    here[me["col"]] = peak
    spot = here.at[me["col"]]
    exchange("col", lambda to: spot, lambda step: spot)
    exchange("row", lambda to: here, lambda step: here)
    all_ref[...] = row_all[...]


def peaks(stats):
    rows, cols, two, lanes = stats.shape
    n = two // 2
    sends = 2 * (rows - 1) + 2 * (cols - 1)
    vmem = pl.BlockSpec(memory_space=pltpu.VMEM)
    return pl.pallas_call(
        peaks_kernel,
        out_shape=[
            jax.ShapeDtypeStruct((rows, cols, n, lanes), jnp.float32),
            jax.ShapeDtypeStruct((two, lanes), jnp.float32),
        ],
        in_specs=[vmem],
        out_specs=[vmem, vmem],
        scratch_shapes=[
            pltpu.VMEM((rows - 1, cols, two, lanes), jnp.float32),
            pltpu.VMEM((cols, two, lanes), jnp.float32),
            pltpu.VMEM((cols - 1, two, lanes), jnp.float32),
            pltpu.VMEM((rows, cols, n, lanes), jnp.float32),
            pltpu.SemaphoreType.DMA((sends,)),
            pltpu.SemaphoreType.DMA((sends,)),
        ],
        compiler_params=pltpu.CompilerParams(collective_id=0, has_side_effects=True),
        name="peaks",
    )(stats)


def body(queries, key_cache, value_cache, key_table, value_table, lengths, token_ids):
    users, beam_part, width_part = queries.shape
    heads_part = width_part // HD
    kv_part = heads_part // GROUP
    rows, cols = lax.axis_size("row"), lax.axis_size("col")
    row_at, col_at = lax.axis_index("row"), lax.axis_index("col")
    positions = key_cache.shape[1]
    offset = (row_at * cols + col_at) * positions
    live = jnp.clip(lengths - offset, 0, positions)
    piece = heads_part * beam_part
    q_local = queries.reshape(users, beam_part, heads_part, HD).transpose(0, 2, 1, 3)
    q_local = q_local.reshape(users, piece, HD)
    some = users // CHUNKS

    gathered = [
        lax.all_gather(lax.all_gather(q_local[i * some : (i + 1) * some], "col"), "row")
        for i in range(CHUNKS)
    ]

    own_keys, own_values = (
        jnp.einsum(
            "uwv,vc->uwc",
            (token_ids[..., None] == jnp.arange(table.shape[0], dtype=jnp.int32)).astype(jnp.bfloat16),
            lax.dynamic_slice_in_dim(table, col_at * kv_part * HD, kv_part * HD, 1),
            preferred_element_type=jnp.float32,
        )
        .reshape(users, beam_part, kv_part, HD)
        .transpose(0, 2, 1, 3)[:, :, None]
        for table in (key_table, value_table)
    )
    q_heads = q_local.astype(jnp.float32).reshape(users, kv_part, GROUP, beam_part, HD)
    own_score = jnp.sum(q_heads * own_keys, axis=-1) * (HD ** (-0.5) * LOG2E)

    sent, owns = [], []
    for i in range(CHUNKS):
        span = slice(i * some, (i + 1) * some)
        numer, m, l = attend(
            live[span],
            gathered[i],
            key_cache,
            value_cache,
            i * some,
        )

        def by_device(x):
            x = x.reshape(some, cols, kv_part, rows, piece // kv_part)
            return x.transpose(3, 1, 0, 2, 4).reshape(rows, cols, some * piece // HD, HD)

        m = by_device(m)
        peak_all, own = peaks(jnp.concatenate([m, by_device(l)], axis=2))
        factor = jnp.exp2(m - peak_all).reshape(rows, cols, some, piece)
        weighted = numer.astype(jnp.float32) * factor[..., None]
        sent.append(
            lax.psum_scatter(weighted.astype(jnp.bfloat16), "row", scatter_dimension=0, tiled=False)
        )
        owns.append(own.reshape(2, some, kv_part, GROUP, beam_part))

    numer = lax.psum_scatter(jnp.concatenate(sent, axis=1), "col", scatter_dimension=0, tiled=False)
    numer = numer.astype(jnp.float32).reshape(users, kv_part, GROUP, beam_part, HD)
    peak, total = jnp.concatenate(owns, axis=1)
    top = jnp.maximum(peak, own_score)
    carried = jnp.exp2(peak - top)
    fresh = jnp.exp2(own_score - top)
    numer = numer * carried[..., None] + fresh[..., None] * own_values
    result = numer / (total * carried + fresh)[..., None]
    result = result.reshape(users, heads_part, beam_part, HD)
    return result.transpose(0, 2, 1, 3).reshape(users, beam_part, width_part).astype(jnp.bfloat16)


def solution(mesh):
    return jax.shard_map(
        body,
        mesh=mesh,
        in_specs=(
            P(None, "row", "col"),
            P(None, ("row", "col"), None),
            P(None, ("row", "col"), None),
            P(),
            P(),
            P(),
            P(None, "row"),
        ),
        out_specs=P(None, "row", "col"),
        check_vma=False,
    )
```
